32 devices in a mesh: table: 4 (over y, core), batch: 8 (over z, x).
Axes of the slice: x: 2, y: 2, z: 4, core: 2. Of those that a mesh axis runs over, the one named last changes fastest.
Arguments:
- emb: bfloat16 [4, 262144, 128], P('table', 'batch'), may hold values from -6 to 6
- short_rows: int32 [192, 4, 32], P(('table', 'batch')), may hold values from 0 to 262143
- short_len: int32 [192, 4], P(('table', 'batch')), may hold values from 1 to 32
- short_sample: int32 [192, 4], P(('table', 'batch')), may hold values from 0 to 7, as said below
- long_rows: int32 [64, 4, 512], P(('table', 'batch')), may hold values from 0 to 262143, as said below
- long_len: int32 [64, 4], P(('table', 'batch')), may hold values from 33 to 500, as said below
- long_sample: int32 [64, 4], P(('table', 'batch')), may hold values from 0 to 7, as said below
Outputs:
- pooled: float32 [256, 4, 128], P(('table', 'batch'))
The draws below stay inside these ranges and needn't reach their ends.
Inputs may be any that keep to these rules, and one draw needn't show every extreme that they name: For each block of 6 short bags and 2 long bags with the same j // 6 and j // 2, and each table, short_sample and long_sample together name each of the 8 samples exactly once. `long_sample`: see short_sample. `long_rows`: within one bag no row id stands more than 256 times among the first long_len positions, and in every draw some bag has a row id that stands exactly that often. `long_len`: in every draw some long bag has length 500.
All inputs are finite; a program needn't handle non-finite values.
Results may differ from the reference program's by a relative error of at most 0.0003.
Values sent between devices are 32-bit elements; how exact they have to be, the bound alone decides.
No kernel may reach another device: no remote copies, remote signals or barrier semaphores. Data moves between devices by JAX's collectives and lax.ppermute only.
A program may use at most 64 MiB of HBM per device.

```python
import jax
import jax.numpy as jnp
from jax import lax

E = 128
B_DEV = 8
WS = 32
WL = 512
MAXLEN = 500
LONG_DEV = 2
SHORT_DEV = 6
R = 262144
NT = 4
B = 256
DEVICES = 32


def bag_order(key):
    scores = jax.random.randint(jax.random.fold_in(key, 7), (DEVICES, NT, B_DEV), 0, 1 << 20, dtype=jnp.int32)
    scores = scores * B_DEV + jnp.arange(B_DEV, dtype=jnp.int32)
    return jnp.argsort(scores, axis=2).astype(jnp.int32)


def draw_short_sample(key, part):
    order = bag_order(key)[:, :, :SHORT_DEV]
    return jnp.transpose(order, (0, 2, 1)).reshape(DEVICES * SHORT_DEV, NT)


def draw_long_sample(key, part):
    order = bag_order(key)[:, :, SHORT_DEV:]
    return jnp.transpose(order, (0, 2, 1)).reshape(DEVICES * LONG_DEV, NT)


def long_bags(key):
    bag_count = DEVICES * LONG_DEV
    total = bag_count * NT
    ceiling = min(256, MAXLEN)
    middle_low = min(17, ceiling)
    middle_high = min(255, ceiling)
    base = jax.random.fold_in(key, 11)
    lengths = jax.random.randint(jax.random.fold_in(base, 1), (bag_count, NT), WS + 1, MAXLEN + 1, dtype=jnp.int32)
    bag_rank = jax.random.permutation(jax.random.fold_in(base, 2), total).astype(jnp.int32).reshape(bag_count, NT)
    middle = jax.random.randint(jax.random.fold_in(base, 3), (bag_count, NT), middle_low, middle_high + 1, dtype=jnp.int32)
    repeats = jnp.where(bag_rank == 0, ceiling, jnp.where(bag_rank <= 15, middle, 0)).astype(jnp.int32)
    lengths = jnp.where(bag_rank == 0, MAXLEN, jnp.maximum(lengths, repeats)).astype(jnp.int32)
    chosen = jax.random.randint(jax.random.fold_in(base, 4), (bag_count, NT), 0, R, dtype=jnp.int32)
    others = jax.random.randint(jax.random.fold_in(base, 5), (bag_count, NT, WL), 0, R - 1, dtype=jnp.int32)
    others = (chosen[:, :, None] + 1 + others) % R
    place = jnp.arange(WL, dtype=jnp.int32)[None, None, :]
    scores = jax.random.randint(jax.random.fold_in(base, 6), (bag_count, NT, WL), 0, 1 << 20, dtype=jnp.int32)
    scores = scores * WL + place
    scores = jnp.where(place < lengths[:, :, None], scores, scores + (1 << 30))
    order = jnp.argsort(scores, axis=2).astype(jnp.int32)
    position_rank = jnp.argsort(order, axis=2).astype(jnp.int32)
    rows = jnp.where(position_rank < repeats[:, :, None], chosen[:, :, None], others)
    return (rows.astype(jnp.int32), lengths.astype(jnp.int32))


def draw_long_rows(key, part):
    return long_bags(key)[0]


def draw_long_len(key, part):
    return long_bags(key)[1]


def plant(entries, rng, least, largest):
    dims = entries.shape
    spot = [jax.random.randint(jax.random.fold_in(rng, axis), (), 0, dims[axis]) for axis in range(len(dims))]
    entries = entries.at[tuple(spot)].set(least)
    longest = dims.index(max(dims))
    spot[longest] = (spot[longest] + 1) % dims[longest]
    return entries.at[tuple(spot)].set(largest)


def levels(own_key, dims, split, low, high):
    level, own = 1.0, jax.random.fold_in(own_key, 6)
    for dim, parts in split:
        steps = jnp.exp(jax.random.uniform(jax.random.fold_in(own, dim), (parts,), jnp.float32, low / len(split), high / len(split)))
        level = level * jnp.repeat(steps, dims[dim] // parts).reshape([-1 if axis == dim else 1 for axis in range(len(dims))])
    return level


def noise(own_key, shape, scale, reach, cuts=(), kind=jnp.bfloat16):
    result = jax.random.normal(own_key, shape, jnp.float32) * scale
    if len(cuts) > 0:
        result = levels(own_key, shape, cuts, -0.22, 0.18) * result
    return jnp.clip(result, min=-reach, max=reach).astype(kind)


def setup_inputs(seed: int = 0) -> dict:
    seeds = jax.random.split(jax.random.key(seed), 8)
    emb = noise(seeds[0], (NT, R, E), 1.0, 6.0, ((0, 4), (1, 8)))
    short_rows = plant(jax.random.randint(seeds[1], (DEVICES * SHORT_DEV, NT, WS), 0, R), jax.random.fold_in(seeds[1], 1), 0, R - 1).astype(jnp.int32)
    short_len = plant(jax.random.randint(seeds[2], (DEVICES * SHORT_DEV, NT), 1, WS + 1), jax.random.fold_in(seeds[2], 1), 1, WS).astype(jnp.int32)
    short_sample = draw_short_sample(jax.random.fold_in(seeds[7], 71), 0)
    long_rows = draw_long_rows(jax.random.fold_in(seeds[7], 71), 0)
    long_len = draw_long_len(jax.random.fold_in(seeds[7], 71), 0)
    long_sample = draw_long_sample(jax.random.fold_in(seeds[7], 71), 0)
    return {"emb": emb, "short_rows": short_rows, "short_len": short_len, "short_sample": short_sample, "long_rows": long_rows, "long_len": long_len, "long_sample": long_sample}


def bag_sums(table, rows, lengths):
    place = jnp.arange(rows.shape[1], dtype=jnp.int32)
    valid = place[None, :] < lengths[:, None]
    picked = table[rows].astype(jnp.float32)
    total = lax.optimization_barrier(jnp.sum(jnp.where(valid[:, :, None], picked, jnp.float32(0.0)), axis=1))
    return total / jnp.sqrt(lengths.astype(jnp.float32))[:, None]

def reference(emb, short_rows, short_len, short_sample, long_rows, long_len, long_sample):
    pooled = jnp.zeros((B, NT, E), jnp.float32)
    short_owner = jnp.arange(DEVICES * SHORT_DEV, dtype=jnp.int32) // SHORT_DEV * B_DEV
    long_owner = jnp.arange(DEVICES * LONG_DEV, dtype=jnp.int32) // LONG_DEV * B_DEV
    for table_id in range(NT):
        short_vec = bag_sums(emb[table_id], short_rows[:, table_id, :], short_len[:, table_id])
        pooled = pooled.at[short_owner + short_sample[:, table_id], table_id].set(short_vec)
        long_vec = bag_sums(emb[table_id], long_rows[:, table_id, :], long_len[:, table_id])
        pooled = pooled.at[long_owner + long_sample[:, table_id], table_id].set(long_vec)
    return pooled
```

```python
import functools

import jax
import jax.numpy as jnp
from jax import lax
from jax.experimental import pallas as pl
from jax.experimental.pallas import tpu as pltpu
from jax.sharding import PartitionSpec as P

LOW = 256
LANES = 128
SUB = 8


def pool_kernel(base_ref, ids_ref, table_hbm, out_ref, table_ref, key_ref, low_ref, counts_ref, sem,
                *, senders, slots, short_bags, width, long_bags, long_width, pitch):
    rows_dev = table_ref.shape[0]
    highs = rows_dev // LOW
    short_span = slots * width
    half = highs * pitch

    load = pltpu.make_async_copy(table_hbm, table_ref, sem)

    @pl.when(pl.program_id(0) == 0)
    def _():
        load.start()

    local = ids_ref[...] - base_ref[0]
    inside = (local >= 0) & (local < rows_dev)
    high = local // LOW
    place = lax.broadcasted_iota(jnp.int32, local.shape, 1)
    key = jnp.where(place < short_span, high * slots + place // width, high)
    key_ref[...] = jnp.where(inside, key, -1)
    low_ref[...] = local % LOW

    def hot(values, count):
        size = values.shape[1]
        spot = lax.broadcasted_iota(jnp.int32, (count, size), 0)
        return (spot == values).astype(jnp.float32).astype(jnp.bfloat16)

    def tally(key, low, count):
        return lax.dot_general(hot(key, count), hot(low, LOW), (((1,), (1,)), ((), ())),
                               preferred_element_type=jnp.float32)

    def count_sender(s, carry):
        span = pl.ds(0, short_span)
        res = tally(key_ref[pl.ds(s, 1), span], low_ref[pl.ds(s, 1), span], highs * slots)
        for part in range(LOW // LANES):
            piece = res[:, part * LANES:(part + 1) * LANES]
            for h in range(highs):
                row = pl.multiple_of(part * half + h * pitch + s * slots, SUB)
                counts_ref[pl.ds(row, slots), :] = piece[h * slots:(h + 1) * slots, :]
        for bag in range(long_bags):
            span = pl.ds(short_span + bag * long_width, long_width)
            res = tally(key_ref[pl.ds(s, 1), span], low_ref[pl.ds(s, 1), span], highs)
            for part in range(LOW // LANES):
                row = part * half + s * slots + short_bags + bag
                counts_ref[pl.ds(row, highs, stride=pitch), :] = res[:, part * LANES:(part + 1) * LANES]
        return carry

    lax.fori_loop(0, senders, count_sender, 0)

    @pl.when(pl.program_id(0) == 0)
    def _():
        load.wait()

    bags = senders * slots
    step = 4 if highs % 4 == 0 else 1

    def add_rows(index, total):
        pieces = []
        for k in range(step):
            h = index * step + k
            for part in range(LOW // LANES):
                row = pl.multiple_of(part * half + h * pitch, SUB)
                pieces.append(counts_ref[pl.ds(row, bags), :].astype(jnp.bfloat16))
        lhs = jnp.concatenate(pieces, axis=1)
        rhs = table_ref[pl.ds(pl.multiple_of(index * step * LOW, LOW), step * LOW), :]
        return total + jnp.dot(lhs, rhs, preferred_element_type=jnp.float32)

    out_ref[...] = lax.fori_loop(0, highs // step, add_rows, jnp.zeros(out_ref.shape, jnp.float32))


def pool(ids, table, row_base, slots, short_bags, width, long_bags, long_width):
    count, span = ids.shape
    senders = min(32, count)
    rows_dev, dim = table.shape
    highs = rows_dev // LOW
    bags = senders * slots
    pitch = bags + SUB
    body = functools.partial(pool_kernel, senders=senders, slots=slots, short_bags=short_bags, width=width,
                             long_bags=long_bags, long_width=long_width, pitch=pitch)
    return pl.pallas_call(
        body,
        out_shape=jax.ShapeDtypeStruct((count * slots, dim), jnp.float32),
        grid=(count // senders,),
        in_specs=[
            pl.BlockSpec(memory_space=pltpu.SMEM),
            pl.BlockSpec((senders, span), lambda i: (i, 0)),
            pl.BlockSpec(memory_space=pl.ANY),
        ],
        out_specs=pl.BlockSpec((bags, dim), lambda i: (i, 0)),
        scratch_shapes=[
            pltpu.VMEM((rows_dev, dim), table.dtype),
            pltpu.VMEM((senders, span), jnp.int32),
            pltpu.VMEM((senders, span), jnp.int32),
            pltpu.VMEM((LOW // LANES * highs * pitch, LANES), jnp.float32),
            pltpu.SemaphoreType.DMA,
        ],
        compiler_params=pltpu.CompilerParams(
            dimension_semantics=("arbitrary",), vmem_limit_bytes=56 * 2**20),
        name="pool",
    )(row_base, ids, table)


def place_kernel(got_ref, weight_ref, out_ref, *, tables, batch):
    for t in range(tables):
        total = got_ref[t * batch]
        for b in range(1, batch):
            total = total + got_ref[t * batch + b]
        weight = weight_ref[t]
        placed = weight[:, 0:1] * total[0:1, :]
        for j in range(1, total.shape[0]):
            placed = placed + weight[:, j:j + 1] * total[j:j + 1, :]
        out_ref[:, t, :] = placed


def place(got, weight, tables, batch):
    slots, dim = got.shape[1:]
    return pl.pallas_call(
        functools.partial(place_kernel, tables=tables, batch=batch),
        out_shape=jax.ShapeDtypeStruct((slots, tables, dim), jnp.float32),
        name="place",
    )(got, weight)


def mask_rows(rows, lengths):
    spot = lax.broadcasted_iota(jnp.int32, rows.shape, 2)
    return jnp.where(spot < lengths[:, :, None], rows, -1)


def make_on_device(axes, tables, batch):
    devices = tables * batch

    def on_device(emb, short_rows, short_len, short_sample, long_rows, long_len, long_sample):
        short_bags, _, width = short_rows.shape
        long_bags, _, long_width = long_rows.shape
        slots = short_bags + long_bags
        short_keys = mask_rows(short_rows, short_len)
        short_keys = jnp.pad(short_keys, ((0, long_bags), (0, 0), (0, 0)), constant_values=-1)
        long_keys = mask_rows(long_rows, long_len)
        keys = jnp.concatenate(
            [jnp.transpose(short_keys, (1, 0, 2)).reshape(tables, slots * width),
             jnp.transpose(long_keys, (1, 0, 2)).reshape(tables, long_bags * long_width)], axis=1)
        span = keys.shape[1]
        sent = jnp.broadcast_to(keys[:, None, :], (tables, batch, span)).reshape(devices, span)
        ids = lax.all_to_all(sent, axes, split_axis=0, concat_axis=0, tiled=True)
        row_base = (lax.axis_index(axes[1]) * emb.shape[1]).astype(jnp.int32).reshape(1)
        part = pool(ids, emb[0], row_base, slots, short_bags, width, long_bags, long_width)
        got = lax.all_to_all(part.reshape(devices, slots, part.shape[1]), axes,
                             split_axis=0, concat_axis=0, tiled=True)
        sample = jnp.concatenate([short_sample, long_sample], axis=0)
        length = jnp.concatenate([short_len, long_len], axis=0).astype(jnp.float32)
        spot = lax.broadcasted_iota(jnp.int32, (tables, slots, slots), 1)
        weight = jnp.where(spot == sample.T[:, None, :], 1.0 / jnp.sqrt(length.T)[:, None, :], 0.0)
        return place(got, weight, tables, batch)

    return on_device


def solution(mesh):
    axes = ("table", "batch")
    return jax.shard_map(
        make_on_device(axes, mesh.shape["table"], mesh.shape["batch"]),
        mesh=mesh,
        in_specs=(
            P("table", "batch", None),
            P(("table", "batch"), None, None),
            P(("table", "batch"), None),
            P(("table", "batch"), None),
            P(("table", "batch"), None, None),
            P(("table", "batch"), None),
            P(("table", "batch"), None),
        ),
        out_specs=P(("table", "batch"), None, None),
        check_vma=False,
    )
```

```python
import functools

import jax
import jax.numpy as jnp
from jax import lax
from jax.experimental import pallas as pl
from jax.experimental.pallas import tpu as pltpu
from jax.sharding import PartitionSpec as P

LOW = 256
LANES = 128
SUB = 8
PACK = 16
UNROLL = 4
LOW_BITS = 8
HOT = jnp.float8_e4m3fn


def pool_kernel(base_ref, ids_ref, table_hbm, out_ref, table_ref, counts_ref, sem,
                *, senders, slots, short_bags, width, long_bags, long_width, pitch):
    rows_dev = table_ref.shape[0]
    highs = rows_dev // LOW
    short_span = slots * width
    half = highs * pitch
    group = pl.program_id(0)

    load = pltpu.make_async_copy(table_hbm, table_ref, sem)

    @pl.when(group == 0)
    def _():
        load.start()

    one = jnp.ones((), jnp.bfloat16)
    zero = jnp.zeros((), jnp.bfloat16)

    def spread(values):
        return jnp.broadcast_to(values, (PACK, values.shape[1]))

    def hot(offsets, count, step):
        offsets = offsets.astype(jnp.bfloat16)
        blocks = [jnp.where(offsets == jnp.asarray(j * step, jnp.bfloat16), one, zero) for j in range(count)]
        return jnp.concatenate(blocks, axis=0).astype(HOT)

    def tally(left, right):
        return lax.dot_general(left, right, (((1,), (1,)), ((), ())), preferred_element_type=jnp.float32)

    def count_sender(s, carry):
        local = ids_ref[group * senders + s] - base_ref[0]
        inside = (local >= 0) & (local < rows_dev)
        high = jnp.where(inside, local >> LOW_BITS, -64).astype(jnp.float32)
        low = (local & (LOW - 1)).astype(jnp.float32)

        def row_of(size):
            return lax.broadcasted_iota(jnp.int32, (PACK, size), 0)

        def low_hot(start, size):
            return hot(spread(low[:, start:start + size]) - row_of(size).astype(jnp.float32), LOW // PACK, PACK)

        row = row_of(short_span)
        bag_of = lax.broadcasted_iota(jnp.int32, (PACK, short_span), 1) // width
        per = PACK // slots
        offsets = jnp.where(row % slots == bag_of,
                            spread(high[:, :short_span]) - (row // slots).astype(jnp.float32), -64.0)
        res = tally(hot(offsets, highs // per, per), low_hot(0, short_span))
        for part in range(LOW // LANES):
            piece = res[:, part * LANES:(part + 1) * LANES]
            for h in range(highs):
                at = pl.multiple_of(part * half + h * pitch + s * slots, SUB)
                counts_ref[pl.ds(at, slots), :] = piece[h * slots:(h + 1) * slots, :]
        for bag in range(long_bags):
            start = short_span + bag * long_width
            offsets = spread(high[:, start:start + long_width]) - row_of(long_width).astype(jnp.float32)
            res = tally(hot(offsets, highs // PACK, PACK), low_hot(start, long_width))
            for part in range(LOW // LANES):
                at = part * half + s * slots + short_bags + bag
                counts_ref[pl.ds(at, highs, stride=pitch), :] = res[:, part * LANES:(part + 1) * LANES]
        return carry

    def count_senders(index, carry):
        for k in range(UNROLL):
            count_sender(index * UNROLL + k, carry)
        return carry

    lax.fori_loop(0, senders // UNROLL, count_senders, 0)

    @pl.when(group == 0)
    def _():
        load.wait()

    bags = senders * slots
    step = 8 if highs % 8 == 0 else 1

    def add_rows(index, total):
        pieces = []
        for k in range(step):
            h = index * step + k
            for part in range(LOW // LANES):
                row = pl.multiple_of(part * half + h * pitch, SUB)
                pieces.append(counts_ref[pl.ds(row, bags), :].astype(jnp.bfloat16))
        lhs = jnp.concatenate(pieces, axis=1)
        rhs = table_ref[pl.ds(pl.multiple_of(index * step * LOW, LOW), step * LOW), :]
        return total + jnp.dot(lhs, rhs, preferred_element_type=jnp.float32)

    out_ref[...] = lax.fori_loop(0, highs // step, add_rows, jnp.zeros(out_ref.shape, jnp.float32))


def pool(ids, table, row_base, slots, short_bags, width, long_bags, long_width):
    count, _, span = ids.shape
    senders = min(32, count)
    rows_dev, dim = table.shape
    highs = rows_dev // LOW
    bags = senders * slots
    pitch = bags + SUB
    body = functools.partial(pool_kernel, senders=senders, slots=slots, short_bags=short_bags, width=width,
                             long_bags=long_bags, long_width=long_width, pitch=pitch)
    return pl.pallas_call(
        body,
        out_shape=jax.ShapeDtypeStruct((count * slots, dim), jnp.float32),
        grid=(count // senders,),
        in_specs=[
            pl.BlockSpec(memory_space=pltpu.SMEM),
            pl.BlockSpec(memory_space=pltpu.VMEM),
            pl.BlockSpec(memory_space=pl.ANY),
        ],
        out_specs=pl.BlockSpec((bags, dim), lambda i: (i, 0)),
        scratch_shapes=[
            pltpu.VMEM((rows_dev, dim), table.dtype),
            pltpu.VMEM((LOW // LANES * highs * pitch, LANES), jnp.float32),
            pltpu.SemaphoreType.DMA,
        ],
        compiler_params=pltpu.CompilerParams(
            dimension_semantics=("arbitrary",), vmem_limit_bytes=56 * 2**20),
        name="pool",
    )(row_base, ids, table)


def place_kernel(got_ref, weight_ref, out_ref, *, tables, batch):
    for t in range(tables):
        total = got_ref[t * batch]
        for b in range(1, batch):
            total = total + got_ref[t * batch + b]
        weight = weight_ref[t]
        placed = weight[:, 0:1] * total[0:1, :]
        for j in range(1, total.shape[0]):
            placed = placed + weight[:, j:j + 1] * total[j:j + 1, :]
        out_ref[:, t, :] = placed


def place(got, weight, tables, batch):
    slots, dim = got.shape[1:]
    return pl.pallas_call(
        functools.partial(place_kernel, tables=tables, batch=batch),
        out_shape=jax.ShapeDtypeStruct((slots, tables, dim), jnp.float32),
        in_specs=[pl.BlockSpec(memory_space=pltpu.VMEM), pl.BlockSpec(memory_space=pltpu.VMEM)],
        out_specs=pl.BlockSpec(memory_space=pltpu.VMEM),
        name="place",
    )(got, weight)


def key_kernel(short_len_ref, long_len_ref, short_ref, long_ref, out_ref, *, batch):
    short_bags, tables, width = short_ref.shape
    long_bags, _, long_width = long_ref.shape
    for t in range(tables):
        pieces = []
        for j in range(short_bags):
            spot = lax.broadcasted_iota(jnp.int32, (1, width), 1)
            pieces.append(jnp.where(spot < short_len_ref[t, j], short_ref[j, t:t + 1, :], -1))
        pieces.append(jnp.full((1, long_bags * width), -1, jnp.int32))
        for j in range(long_bags):
            spot = lax.broadcasted_iota(jnp.int32, (1, long_width), 1)
            pieces.append(jnp.where(spot < long_len_ref[j, t], long_ref[j, t:t + 1, :], -1))
        row = jnp.concatenate(pieces, axis=1)
        for b in range(batch):
            out_ref[t * batch + b] = row


def make_keys(short_rows, short_len, long_rows, long_len, batch):
    short_bags, tables, width = short_rows.shape
    long_bags, _, long_width = long_rows.shape
    span = (short_bags + long_bags) * width + long_bags * long_width
    return pl.pallas_call(
        functools.partial(key_kernel, batch=batch),
        out_shape=jax.ShapeDtypeStruct((tables * batch, 1, span), jnp.int32),
        in_specs=[
            pl.BlockSpec(memory_space=pltpu.SMEM),
            pl.BlockSpec(memory_space=pltpu.SMEM),
            pl.BlockSpec(memory_space=pltpu.VMEM),
            pl.BlockSpec(memory_space=pltpu.VMEM),
        ],
        out_specs=pl.BlockSpec(memory_space=pltpu.VMEM),
        name="keys",
    )(short_len.T, long_len, short_rows, long_rows)


def make_on_device(axes, tables, batch):
    devices = tables * batch

    def on_device(emb, short_rows, short_len, short_sample, long_rows, long_len, long_sample):
        short_bags, _, width = short_rows.shape
        long_bags, _, long_width = long_rows.shape
        slots = short_bags + long_bags
        sent = make_keys(short_rows, short_len, long_rows, long_len, batch)
        ids = lax.all_to_all(sent, axes, split_axis=0, concat_axis=0, tiled=True)
        row_base = (lax.axis_index(axes[1]) * emb.shape[1]).astype(jnp.int32).reshape(1)
        part = pool(ids, emb[0], row_base, slots, short_bags, width, long_bags, long_width)
        got = lax.all_to_all(part.reshape(devices, slots, part.shape[1]), axes,
                             split_axis=0, concat_axis=0, tiled=True)
        sample = jnp.concatenate([short_sample, long_sample], axis=0)
        length = jnp.concatenate([short_len, long_len], axis=0).astype(jnp.float32)
        spot = lax.broadcasted_iota(jnp.int32, (tables, slots, slots), 1)
        weight = jnp.where(spot == sample.T[:, None, :], 1.0 / jnp.sqrt(length.T)[:, None, :], 0.0)
        return place(got, weight, tables, batch)

    return on_device


def solution(mesh):
    axes = ("table", "batch")
    return jax.shard_map(
        make_on_device(axes, mesh.shape["table"], mesh.shape["batch"]),
        mesh=mesh,
        in_specs=(
            P("table", "batch", None),
            P(("table", "batch"), None, None),
            P(("table", "batch"), None),
            P(("table", "batch"), None),
            P(("table", "batch"), None, None),
            P(("table", "batch"), None),
            P(("table", "batch"), None),
        ),
        out_specs=P(("table", "batch"), None, None),
        check_vma=False,
    )
```

```python
import functools

import jax
import jax.numpy as jnp
from jax import lax
from jax.experimental import pallas as pl
from jax.experimental.pallas import tpu as pltpu
from jax.sharding import PartitionSpec as P

LOW = 256
LANES = 128
SUB = 8
PACK = 16
UNROLL = 4
LOW_BITS = 8
HOT = jnp.float8_e4m3fn


def pool_kernel(base_ref, ids_ref, table_hbm, out_ref, table_ref, counts_ref, sem,
                *, senders, slots, short_bags, width, long_bags, long_width, pitch):
    rows_dev = table_ref.shape[0]
    highs = rows_dev // LOW
    short_span = slots * width
    half = highs * pitch
    group = pl.program_id(0)

    load = pltpu.make_async_copy(table_hbm, table_ref, sem)

    @pl.when(group == 0)
    def _():
        load.start()

    one = jnp.ones((), jnp.bfloat16)
    zero = jnp.zeros((), jnp.bfloat16)

    def spread(values):
        return jnp.broadcast_to(values, (PACK, values.shape[1]))

    def hot(offsets, count, step):
        offsets = offsets.astype(jnp.bfloat16)
        blocks = [jnp.where(offsets == jnp.asarray(j * step, jnp.bfloat16), one, zero) for j in range(count)]
        return jnp.concatenate(blocks, axis=0).astype(HOT)

    def tally(left, right):
        return lax.dot_general(left, right, (((1,), (1,)), ((), ())), preferred_element_type=jnp.float32)

    def count_sender(s, carry):
        local = ids_ref[group * senders + s] - base_ref[0]
        inside = (local >= 0) & (local < rows_dev)
        high = jnp.where(inside, local >> LOW_BITS, -64).astype(jnp.float32)
        low = (local & (LOW - 1)).astype(jnp.float32)

        def row_of(size):
            return lax.broadcasted_iota(jnp.int32, (PACK, size), 0)

        def low_hot(start, size):
            return hot(spread(low[:, start:start + size]) - row_of(size).astype(jnp.float32), LOW // PACK, PACK)

        row = row_of(short_span)
        bag_of = lax.broadcasted_iota(jnp.int32, (PACK, short_span), 1) // width
        per = PACK // slots
        offsets = jnp.where(row % slots == bag_of,
                            spread(high[:, :short_span]) - (row // slots).astype(jnp.float32), -64.0)
        res = tally(hot(offsets, highs // per, per), low_hot(0, short_span))
        for part in range(LOW // LANES):
            piece = res[:, part * LANES:(part + 1) * LANES]
            for h in range(highs):
                at = pl.multiple_of(part * half + h * pitch + s * slots, SUB)
                counts_ref[pl.ds(at, slots), :] = piece[h * slots:(h + 1) * slots, :]
        for bag in range(long_bags):
            start = short_span + bag * long_width
            offsets = spread(high[:, start:start + long_width]) - row_of(long_width).astype(jnp.float32)
            res = tally(hot(offsets, highs // PACK, PACK), low_hot(start, long_width))
            for part in range(LOW // LANES):
                at = part * half + s * slots + short_bags + bag
                counts_ref[pl.ds(at, highs, stride=pitch), :] = res[:, part * LANES:(part + 1) * LANES]
        return carry

    def count_senders(index, carry):
        for k in range(UNROLL):
            count_sender(index * UNROLL + k, carry)
        return carry

    lax.fori_loop(0, senders // UNROLL, count_senders, 0)

    @pl.when(group == 0)
    def _():
        load.wait()

    bags = senders * slots
    step = 8 if highs % 8 == 0 else 1

    def add_rows(index, total):
        pieces = []
        for k in range(step):
            h = index * step + k
            for part in range(LOW // LANES):
                row = pl.multiple_of(part * half + h * pitch, SUB)
                pieces.append(counts_ref[pl.ds(row, bags), :].astype(jnp.bfloat16))
        lhs = jnp.concatenate(pieces, axis=1)
        rhs = table_ref[pl.ds(pl.multiple_of(index * step * LOW, LOW), step * LOW), :]
        return total + jnp.dot(lhs, rhs, preferred_element_type=jnp.float32)

    out_ref[...] = lax.fori_loop(0, highs // step, add_rows, jnp.zeros(out_ref.shape, jnp.float32))


def pool(ids, table, row_base, slots, short_bags, width, long_bags, long_width):
    count, _, span = ids.shape
    senders = min(32, count)
    rows_dev, dim = table.shape
    highs = rows_dev // LOW
    bags = senders * slots
    pitch = bags + SUB
    body = functools.partial(pool_kernel, senders=senders, slots=slots, short_bags=short_bags, width=width,
                             long_bags=long_bags, long_width=long_width, pitch=pitch)
    return pl.pallas_call(
        body,
        out_shape=jax.ShapeDtypeStruct((count * slots, dim), jnp.float32),
        grid=(count // senders,),
        in_specs=[
            pl.BlockSpec(memory_space=pltpu.SMEM),
            pl.BlockSpec(memory_space=pltpu.VMEM),
            pl.BlockSpec(memory_space=pl.ANY),
        ],
        out_specs=pl.BlockSpec((bags, dim), lambda i: (i, 0)),
        scratch_shapes=[
            pltpu.VMEM((rows_dev, dim), table.dtype),
            pltpu.VMEM((LOW // LANES * highs * pitch, LANES), jnp.float32),
            pltpu.SemaphoreType.DMA,
        ],
        compiler_params=pltpu.CompilerParams(
            dimension_semantics=("arbitrary",), vmem_limit_bytes=56 * 2**20),
        name="pool",
    )(row_base, pltpu.with_memory_space_constraint(ids, pltpu.VMEM), table)


def place_kernel(got_ref, weight_ref, out_ref, *, tables, batch):
    for t in range(tables):
        total = got_ref[t * batch]
        for b in range(1, batch):
            total = total + got_ref[t * batch + b]
        weight = weight_ref[t]
        placed = weight[:, 0:1] * total[0:1, :]
        for j in range(1, total.shape[0]):
            placed = placed + weight[:, j:j + 1] * total[j:j + 1, :]
        out_ref[:, t, :] = placed


def place(got, weight, tables, batch):
    slots, dim = got.shape[1:]
    return pl.pallas_call(
        functools.partial(place_kernel, tables=tables, batch=batch),
        out_shape=jax.ShapeDtypeStruct((slots, tables, dim), jnp.float32),
        in_specs=[pl.BlockSpec(memory_space=pltpu.VMEM), pl.BlockSpec(memory_space=pltpu.VMEM)],
        out_specs=pl.BlockSpec(memory_space=pltpu.VMEM),
        name="place",
    )(pltpu.with_memory_space_constraint(got, pltpu.VMEM), weight)


def key_kernel(short_len_ref, long_len_ref, short_ref, long_ref, out_ref, *, batch):
    short_bags, tables, width = short_ref.shape
    long_bags, _, long_width = long_ref.shape
    for t in range(tables):
        pieces = []
        for j in range(short_bags):
            spot = lax.broadcasted_iota(jnp.int32, (1, width), 1)
            pieces.append(jnp.where(spot < short_len_ref[t, j], short_ref[j, t:t + 1, :], -1))
        pieces.append(jnp.full((1, long_bags * width), -1, jnp.int32))
        for j in range(long_bags):
            spot = lax.broadcasted_iota(jnp.int32, (1, long_width), 1)
            pieces.append(jnp.where(spot < long_len_ref[j, t], long_ref[j, t:t + 1, :], -1))
        row = jnp.concatenate(pieces, axis=1)
        for b in range(batch):
            out_ref[t * batch + b] = row


def make_keys(short_rows, short_len, long_rows, long_len, batch):
    short_bags, tables, width = short_rows.shape
    long_bags, _, long_width = long_rows.shape
    span = (short_bags + long_bags) * width + long_bags * long_width
    return pl.pallas_call(
        functools.partial(key_kernel, batch=batch),
        out_shape=jax.ShapeDtypeStruct((tables * batch, 1, span), jnp.int32),
        in_specs=[
            pl.BlockSpec(memory_space=pltpu.SMEM),
            pl.BlockSpec(memory_space=pltpu.SMEM),
            pl.BlockSpec(memory_space=pltpu.VMEM),
            pl.BlockSpec(memory_space=pltpu.VMEM),
        ],
        out_specs=pl.BlockSpec(memory_space=pltpu.VMEM),
        name="keys",
    )(short_len.T, long_len, short_rows, long_rows)


def make_on_device(axes, tables, batch):
    devices = tables * batch

    def on_device(emb, short_rows, short_len, short_sample, long_rows, long_len, long_sample):
        short_bags, _, width = short_rows.shape
        long_bags, _, long_width = long_rows.shape
        slots = short_bags + long_bags
        sent = make_keys(short_rows, short_len, long_rows, long_len, batch)
        ids = lax.all_to_all(sent, axes, split_axis=0, concat_axis=0, tiled=True)
        row_base = (lax.axis_index(axes[1]) * emb.shape[1]).astype(jnp.int32).reshape(1)
        part = pool(ids, emb[0], row_base, slots, short_bags, width, long_bags, long_width)
        got = lax.all_to_all(part.reshape(devices, slots, part.shape[1]), axes,
                             split_axis=0, concat_axis=0, tiled=True)
        sample = jnp.concatenate([short_sample, long_sample], axis=0)
        length = jnp.concatenate([short_len, long_len], axis=0).astype(jnp.float32)
        spot = lax.broadcasted_iota(jnp.int32, (tables, slots, slots), 1)
        weight = jnp.where(spot == sample.T[:, None, :], 1.0 / jnp.sqrt(length.T)[:, None, :], 0.0)
        return place(got, weight, tables, batch)

    return on_device


def solution(mesh):
    axes = ("table", "batch")
    return jax.shard_map(
        make_on_device(axes, mesh.shape["table"], mesh.shape["batch"]),
        mesh=mesh,
        in_specs=(
            P("table", "batch", None),
            P(("table", "batch"), None, None),
            P(("table", "batch"), None),
            P(("table", "batch"), None),
            P(("table", "batch"), None, None),
            P(("table", "batch"), None),
            P(("table", "batch"), None),
        ),
        out_specs=P(("table", "batch"), None, None),
        check_vma=False,
    )
```
